256 devices in a mesh: ep: 64 (over x, z, core), tp: 4 (over y).
Axes of the slice: x: 4, y: 4, z: 8, core: 2. Of those that a mesh axis runs over, the one named last changes fastest.
Arguments:
- tokens: bfloat16 [2048, 7168], P('ep', 'tp'), may hold values from -6 to 6
- routes: int32 [2048, 8], P('ep'), may hold values from 0 to 63, all different within a row; in each aligned block of 32 rows (0 to 31, 32 to 63, ...) at most 8 rows name the same one
- route_weights: float32 [2048, 8], P('ep'), may hold values from 0.05 to 1
- gate_proj: bfloat16 [64, 7168, 1024], P('ep', None, 'tp'), may hold values from -0.0625 to 0.0625
- up_proj: bfloat16 [64, 7168, 1024], P('ep', None, 'tp'), may hold values from -0.0625 to 0.0625
- down_proj: bfloat16 [64, 1024, 7168], P('ep', 'tp'), may hold values from -0.1875 to 0.1875
Outputs:
- mixed: bfloat16 [2048, 7168], P('ep', 'tp')
The draws below stay inside these ranges and needn't reach their ends.
Inputs may be any that keep to these rules, and one draw needn't show every extreme that they name: `routes`: each token names 8 different experts; among the 32 tokens of one index of ep no expert is named more than 8 times.
All inputs are finite; a program needn't handle non-finite values.
Results may differ from the reference program's by a relative error of at most 0.012.
Values may be sent and summed in bfloat16 or wider, within the bound.
No kernel may reach another device: no remote copies, remote signals or barrier semaphores. Data moves between devices by JAX's collectives and lax.ppermute only.
A program may use at most 64 MiB of HBM per device.

```python
import math
import jax
import jax.numpy as jnp
import numpy as np
from jax import lax

D = 7168
FF = 1024
TOP = 8
TOK_EP = 32
N_EXP = 64
TOKENS = 2048
CAP = 8
N_EP = 64
N_TP = 4


def shard_levels(rng, shape, split, low, high):
    level, own = 1.0, jax.random.fold_in(rng, 6)
    for dim, blocks in split:
        draws = jnp.exp(jax.random.uniform(jax.random.fold_in(own, dim), (blocks,), jnp.float32, low / len(split), high / len(split)))
        level = level * jnp.repeat(draws, shape[dim] // blocks).reshape([-1 if axis == dim else 1 for axis in range(len(shape))])
    return level


def deal_out(rng, own, number, rows, amount, top, limit, skew):
    sequence = jax.random.permutation(rng, amount)
    packed, ordinary = load_shares(amount, rows * top, limit, skew, True), load_shares(amount, rows * top, limit, skew, False)
    places = jnp.arange(amount)

    def named(tallies, turn):
        used = int((tallies > 0).sum())
        fixed = max(1, used // 4)
        moved = fixed + (places - fixed + turn * (used - fixed)) % max(1, amount - fixed)
        return jnp.zeros((amount,), jnp.int32).at[sequence[jnp.where(places < fixed, places, moved)]].set(jnp.asarray(tallies, jnp.int32))

    tallies = jnp.where(number % 4 == 0, named(packed, number // 4), named(ordinary, number - number // 4 - 1))
    mixed = jax.random.permutation(jax.random.fold_in(own, 3), amount)
    source_of, sink = mixed[0:amount // 2 * 2:2], mixed[1:amount // 2 * 2:2]
    room = jnp.minimum(tallies[source_of] - 1, limit - tallies[sink]) // 2
    room = jnp.where((source_of == sequence[0]) | (sink == sequence[0]) | (tallies[sink] == 0), 0, jnp.maximum(room, 0))
    moved = jax.random.randint(jax.random.fold_in(own, 4), (amount // 2,), 0, 1 << 20) % (room + 1)
    tallies = tallies.at[source_of].add(-moved).at[sink].add(moved)
    members = jnp.searchsorted(jnp.cumsum(tallies), jnp.arange(rows * top), side="right").astype(jnp.int32)
    listing = members.reshape(top, rows).T
    listing = listing[jax.random.permutation(jax.random.fold_in(own, 1), rows)]
    turn = jax.random.randint(jax.random.fold_in(own, 2), (rows, 1), 0, top)
    return jnp.take_along_axis(listing, (jnp.arange(top)[None, :] + turn) % top, axis=1)


def load_shares(number_of, total, limit, skew, full):
    portions = [(1 << 20) // math.isqrt(grade ** skew) + 1 for grade in range(1, number_of + 1)]
    largest = limit if full else min(limit, max(-(-total // number_of), total * portions[0] // sum(portions)))
    least = 1 if total - largest >= number_of - 1 else 0
    holding, rest = [largest] + [least] * (number_of - 1), total - largest - least * (number_of - 1)
    while rest > 0:
        free = [i for i in range(1, number_of) if holding[i] < largest] or [i for i in range(1, number_of) if holding[i] < limit]
        whole, left = sum([portions[i] for i in free]), rest
        for i in free:
            extra = min(limit - holding[i], max(1, left * portions[i] // whole), rest)
            holding[i] = holding[i] + extra
            rest = rest - extra
    return np.array(holding)


def centred(key, extent, width, bound, split=(), kind=jnp.bfloat16):
    array = jax.random.normal(key, extent, jnp.float32) * width
    if len(split) > 0:
        array = shard_levels(key, extent, split, -0.22, 0.18) * array
    return jnp.clip(array, min=-bound, max=bound).astype(kind)


def setup_inputs(seed: int = 0) -> dict:
    splits = jax.random.split(jax.random.key(seed), 7)
    tokens = centred(splits[0], (TOKENS, D), 1.0, 6.0, ((0, 64), (1, 4)))
    routes_keys = jax.random.split(jax.random.fold_in(splits[1], 1), TOKENS // TOK_EP)
    routes_turns = jax.random.permutation(jax.random.fold_in(splits[1], 3), TOKENS // TOK_EP)
    routes = jax.vmap(lambda own, number: deal_out(jax.random.fold_in(splits[1], 2), own, number, TOK_EP, N_EXP, TOP, CAP, 2))(routes_keys, routes_turns).reshape((TOKENS, TOP))
    route_weights = jnp.clip(jnp.exp(math.log(1.0) - 2.9957323 * jax.random.uniform(splits[2], (TOKENS, TOP), jnp.float32) ** shard_levels(splits[2], (TOKENS, TOP), ((0, 64),), -0.2, 0.2)), 0.05, 1.0)
    gate_proj = centred(splits[3], (N_EXP, D, FF), D ** -0.5, 0.0625, ((0, 64), (2, 4)))
    up_proj = centred(splits[4], (N_EXP, D, FF), D ** -0.5, 0.0625, ((0, 64), (2, 4)))
    down_proj = centred(splits[5], (N_EXP, FF, D), FF ** -0.5, 0.1875, ((0, 64), (1, 4)))
    return dict(tokens=tokens, routes=routes, route_weights=route_weights, gate_proj=gate_proj, up_proj=up_proj, down_proj=down_proj)


def run_expert(inputs):
    expert_rows, w_gate, w_up, w_down = inputs
    gate_act = jnp.dot(expert_rows, w_gate, preferred_element_type=jnp.float32)
    up_act = jnp.dot(expert_rows, w_up, preferred_element_type=jnp.float32)
    hidden = (jax.nn.silu(gate_act) * up_act).astype(jnp.bfloat16)
    part_size = FF // N_TP
    totals = jnp.zeros((expert_rows.shape[0], D), jnp.float32)
    for block_index in range(N_TP):
        low = block_index * part_size
        partial_value = jnp.dot(hidden[:, low:low + part_size], w_down[low:low + part_size], preferred_element_type=jnp.float32)
        totals = totals + lax.optimization_barrier(partial_value.astype(jnp.bfloat16)).astype(jnp.float32)
    return totals.astype(jnp.bfloat16)


def reference(tokens, routes, route_weights, gate_proj, up_proj, down_proj):
    per_block = TOK_EP * TOP
    blocks = routes.reshape(N_EP, per_block).astype(jnp.int32)
    onehot = (blocks[:, :, None] == jnp.arange(N_EXP, dtype=jnp.int32)[None, None, :]).astype(jnp.int32)
    before = jnp.cumsum(onehot, axis=1) - onehot
    position = jnp.sum(before * onehot, axis=2).astype(jnp.int32)
    sources = jnp.arange(N_EP, dtype=jnp.int32)[:, None]
    target = (blocks * (N_EP * CAP) + sources * CAP + position).reshape(-1).astype(jnp.int32)
    owners = jnp.repeat(jnp.arange(TOKENS, dtype=jnp.int32), TOP)
    buffer = jnp.zeros((N_EXP * N_EP * CAP, D), jnp.bfloat16).at[target].set(tokens[owners])
    buffer = buffer.reshape(N_EXP, N_EP * CAP, D)
    results = lax.map(run_expert, (buffer, gate_proj, up_proj, down_proj)).reshape(-1, D)
    picked = results[target].astype(jnp.float32).reshape(TOKENS, TOP, D)
    mixed = jnp.sum(picked * route_weights[:, :, None].astype(jnp.float32), axis=1)
    return mixed.astype(jnp.bfloat16)
```

```python
import jax
import jax.numpy as jnp
from jax import lax
from jax.experimental import pallas as pl
from jax.experimental.pallas import tpu as pltpu
from jax.sharding import PartitionSpec as P

CHUNKS = 2


def hidden_kernel(x_ref, gate_ref, up_ref, out_ref, gate_acc, up_acc):
    step = pl.program_id(0)

    @pl.when(step == 0)
    def _():
        gate_acc[...] = jnp.zeros_like(gate_acc)
        up_acc[...] = jnp.zeros_like(up_acc)

    gate_acc[...] += jnp.dot(x_ref[...], gate_ref[...], preferred_element_type=jnp.float32)
    up_acc[...] += jnp.dot(x_ref[...], up_ref[...], preferred_element_type=jnp.float32)

    @pl.when(step == pl.num_programs(0) - 1)
    def _():
        gate = gate_acc[...]
        out_ref[...] = (gate / (1.0 + jnp.exp(-gate)) * up_acc[...]).astype(out_ref.dtype)


def hidden_of(block_in, gate_proj, up_proj):
    rows, width = block_in.shape
    cols = gate_proj.shape[2]
    steps = 4
    depth = width // steps
    weight = pl.BlockSpec((None, depth, cols), lambda k: (0, k, 0))
    return pl.pallas_call(
        hidden_kernel,
        grid=(steps,),
        in_specs=[pl.BlockSpec((rows, depth), lambda k: (0, k)), weight, weight],
        out_specs=pl.BlockSpec((rows, cols), lambda k: (0, 0)),
        out_shape=jax.ShapeDtypeStruct((rows, cols), jnp.bfloat16),
        scratch_shapes=[pltpu.VMEM((rows, cols), jnp.float32)] * 2,
        cost_estimate=pl.CostEstimate(
            flops=4 * rows * width * cols,
            bytes_accessed=2 * rows * width + 4 * width * cols,
            transcendentals=rows * cols,
        ),
        name="hidden",
    )(block_in, gate_proj, up_proj)


def down_kernel(*refs):
    out_ref = refs[-1]
    pairs = (len(refs) - 1) // 2
    total = jnp.dot(refs[0][...], refs[pairs][...], preferred_element_type=jnp.float32)
    for i in range(1, pairs):
        total += jnp.dot(refs[i][...], refs[pairs + i][...], preferred_element_type=jnp.float32)
    out_ref[...] = total.astype(out_ref.dtype)


def down_of(hiddens, downs):
    rows, inner = hiddens[0].shape
    width = downs[0].shape[1]
    steps = 7
    cols = width // steps
    n = len(hiddens)
    return pl.pallas_call(
        down_kernel,
        grid=(steps,),
        in_specs=[pl.BlockSpec((rows, inner), lambda k: (0, 0))] * n
        + [pl.BlockSpec((inner, cols), lambda k: (0, k))] * n,
        out_specs=pl.BlockSpec((rows, cols), lambda k: (0, k)),
        out_shape=jax.ShapeDtypeStruct((rows, width), jnp.bfloat16),
        cost_estimate=pl.CostEstimate(
            flops=2 * n * rows * inner * width,
            bytes_accessed=2 * n * inner * (rows + width) + 2 * rows * width,
            transcendentals=0,
        ),
        name="down",
    )(*hiddens, *downs)


def layer(tokens, routes, route_weights, gate_proj, up_proj, down_proj):
    w_down = down_proj[0]
    tok_count, width = tokens.shape
    fanout = routes.shape[1]
    experts = lax.axis_size("ep")
    parts = lax.axis_size("tp")
    me = lax.axis_index("tp")
    capacity = min(tok_count, max(2, 2 * tok_count * fanout // experts))
    share = capacity // CHUNKS

    def shift(value, by):
        return lax.ppermute(value, "tp", [(i, (i + by) % parts) for i in range(parts)])

    downs = []
    for by in range(parts):
        start = lax.rem(me + by, parts) * width
        piece = lax.dynamic_slice_in_dim(w_down, start, width, axis=1)
        downs.append(piece if by == 0 else shift(piece, by))

    flat_ids = routes.reshape(-1)
    onehot = (flat_ids[:, None] == jnp.arange(experts, dtype=jnp.int32)[None, :]).astype(jnp.int32)
    before = jnp.cumsum(onehot, axis=0) - onehot
    position = jnp.sum(before * onehot, axis=1)
    target = (flat_ids * capacity + position).reshape(tok_count, fanout)

    mixed = jnp.zeros((tok_count, width), jnp.float32)
    for chunk in range(CHUNKS):
        rows = experts * share
        row = jnp.arange(rows, dtype=jnp.int32)
        slot = row // share * capacity + chunk * share + row % share
        select = jnp.any(target[None, :, :] == slot[:, None, None], axis=2).astype(jnp.bfloat16)
        sending = jnp.dot(select, tokens, preferred_element_type=jnp.float32).astype(jnp.bfloat16)
        arrived = lax.all_to_all(
            sending.reshape(experts, share, width), "ep", split_axis=0, concat_axis=0, tiled=True
        )
        arrived = arrived.reshape(rows, width)
        block_in = lax.all_gather(arrived, "tp", axis=1, tiled=True)
        hidden = hidden_of(block_in, gate_proj, up_proj)
        hiddens = [hidden] + [shift(hidden, by) for by in range(1, parts)]
        out = down_of(hiddens, downs)
        back = lax.all_to_all(
            out.reshape(experts, share, width), "ep", split_axis=0, concat_axis=0, tiled=True
        ).reshape(rows, width)
        weight = jnp.sum(
            jnp.where(target[:, :, None] == slot[None, None, :], route_weights[:, :, None], 0.0), axis=1
        )
        high = weight.astype(jnp.bfloat16)
        low = (weight - high.astype(jnp.float32)).astype(jnp.bfloat16)
        both = jnp.dot(jnp.concatenate([high, low]), back, preferred_element_type=jnp.float32)
        mixed = mixed + (both[:tok_count] + both[tok_count:])
    return mixed.astype(jnp.bfloat16)


def solution(mesh):
    in_specs = (
        P("ep", "tp"),
        P("ep", None),
        P("ep", None),
        P("ep", None, "tp"),
        P("ep", None, "tp"),
        P("ep", "tp", None),
    )
    out_specs = P("ep", "tp")
    return jax.shard_map(layer, mesh=mesh, in_specs=in_specs, out_specs=out_specs, check_vma=False)
```

```python
import functools

import jax
import jax.numpy as jnp
from jax import lax
from jax.experimental import pallas as pl
from jax.experimental.pallas import tpu as pltpu
from jax.sharding import PartitionSpec as P


NX, NZ, NC = 4, 8, 2
NEAR = NX * NC
SLOTS = 8
META = 128
TILE = 256
F32 = jnp.float32
BF16 = jnp.bfloat16


def smem():
    return pl.BlockSpec(memory_space=pltpu.SMEM)


def vmem():
    return pl.BlockSpec(memory_space=pltpu.VMEM)


def placing(experts_ref, meta):
    count = meta.shape[0]
    lane = lax.broadcasted_iota(jnp.int32, meta.shape, 1)
    hits = jnp.zeros(meta.shape, F32)
    eqs = []
    for q in range(NEAR):
        eq = (meta == experts_ref[q].astype(F32)) & (lane < SLOTS)
        eqs.append(eq)
        hit = jnp.max(jnp.where(eq, 1.0, 0.0), axis=1, keepdims=True)
        hits = jnp.where(lane == q, hit, hits)
    block = count // NZ
    r = lax.broadcasted_iota(jnp.int32, (count, count), 0)
    c = lax.broadcasted_iota(jnp.int32, (count, count), 1)
    earlier = jnp.where((r // block == c // block) & (c < r), 1.0, 0.0).astype(BF16)
    slots = jnp.dot(earlier, hits.astype(BF16), preferred_element_type=F32)
    slots = jnp.where(hits > 0.5, slots, -1.0)
    return eqs, slots


def spread(values, slots):
    count = slots.shape[0]
    shape = (count, 2 * NZ * SLOTS)
    lane = lax.broadcasted_iota(jnp.int32, shape, 1)
    row = lax.broadcasted_iota(jnp.int32, shape, 0)
    half = NZ * SLOTS
    same = (lane % half) // SLOTS == row // (count // NZ)
    column = (lane % SLOTS).astype(F32)
    parts = []
    for q in range(0, NEAR, 2):
        slot = jnp.where(lane < half, slots[:, q : q + 1], slots[:, q + 1 : q + 2])
        value = jnp.where(lane < half, values[q], values[q + 1])
        parts.append(jnp.where(same & (slot == column), value, 0.0).astype(BF16))
    return jnp.concatenate(parts, axis=1)


def select_kernel(experts_ref, *refs):
    pieces, outs = refs[:NZ], refs[NZ:]
    width = outs[0].shape[1]
    meta = jnp.concatenate([p[:, width:] for p in pieces]).astype(F32)
    _, slots = placing(experts_ref, meta)
    ones = jnp.ones((meta.shape[0], 1), F32)
    mask = spread([ones] * NEAR, slots)
    mask_t = mask.astype(F32).T.astype(BF16)

    @pl.loop(0, width // TILE)
    def _(i):
        at = pl.ds(pl.multiple_of(i * TILE, TILE), TILE)
        rows = jnp.concatenate([p[:, at] for p in pieces])
        sent = jnp.dot(mask_t, rows, preferred_element_type=F32)
        for q in range(NEAR):
            n = NZ * SLOTS
            outs[q][:, at] = sent[q * n : (q + 1) * n].astype(BF16)


def select_of(near, pieces, width):
    out = jax.ShapeDtypeStruct((NZ * SLOTS, width), BF16)
    return pl.pallas_call(
        select_kernel,
        in_specs=[smem()] + [vmem()] * NZ,
        out_specs=[vmem()] * NEAR,
        out_shape=[out] * NEAR,
        cost_estimate=pl.CostEstimate(flops=10**9, bytes_accessed=3 * 10**6, transcendentals=0),
        name="select",
    )(near, *pieces)


def weigh_kernel(experts_ref, *refs):
    pieces, (high_ref, low_ref) = refs[:NZ], refs[NZ:]
    meta = jnp.concatenate([p[:, p.shape[1] - META :] for p in pieces]).astype(F32)
    eqs, slots = placing(experts_ref, meta)
    for order, out_ref in ((1, high_ref), (2, low_ref)):
        moved = pltpu.roll(meta, META - order * SLOTS, 1)
        values = [jnp.sum(jnp.where(eq, moved, 0.0), axis=1, keepdims=True) for eq in eqs]
        out_ref[...] = spread(values, slots)


def weigh_of(near, pieces):
    count = NZ * pieces[0].shape[0]
    out = jax.ShapeDtypeStruct((count, NEAR * NZ * SLOTS), BF16)
    return pl.pallas_call(
        weigh_kernel,
        in_specs=[smem()] + [vmem()] * NZ,
        out_specs=[vmem()] * 2,
        out_shape=[out] * 2,
        cost_estimate=pl.CostEstimate(flops=10**9, bytes_accessed=2 * 10**6, transcendentals=0),
        name="weigh",
    )(near, *pieces)


def hidden_kernel(order_ref, *refs):
    blocks, (gate_ref, up_ref, out_ref, gate_acc, up_acc) = refs[:-5], refs[-5:]
    step = pl.program_id(0)

    @pl.when(step == 0)
    def _():
        gate_acc[...] = jnp.zeros_like(gate_acc)
        up_acc[...] = jnp.zeros_like(up_acc)

    for i, block in enumerate(blocks):

        @pl.when(step == i)
        def _(block=block, i=i):
            size = block.shape[1] // 2

            @pl.loop(0, 2)
            def _(j):
                at = pl.ds(pl.multiple_of(j * size, size), size)
                gate_acc[...] += jnp.dot(block[:, at], gate_ref[at, :], preferred_element_type=F32)
                up_acc[...] += jnp.dot(block[:, at], up_ref[at, :], preferred_element_type=F32)

    @pl.when(step == len(blocks) - 1)
    def _():
        gate = gate_acc[...]
        out_ref[...] = (gate / (1.0 + jnp.exp(-gate)) * up_acc[...]).astype(BF16)


def hidden_of(order, blocks, gate_proj, up_proj):
    rows, depth = blocks[0].shape
    cols = gate_proj.shape[2]
    n = len(blocks)
    weight = pl.BlockSpec((None, depth, cols), lambda k, order: (0, order[k], 0))
    return pl.pallas_call(
        hidden_kernel,
        grid_spec=pltpu.PrefetchScalarGridSpec(
            num_scalar_prefetch=1,
            grid=(n,),
            in_specs=[pl.BlockSpec((rows, depth), lambda k, order: (0, 0))] * n + [weight, weight],
            out_specs=pl.BlockSpec((rows, cols), lambda k, order: (0, 0)),
            scratch_shapes=[pltpu.VMEM((rows, cols), F32)] * 2,
        ),
        out_shape=jax.ShapeDtypeStruct((rows, cols), BF16),
        cost_estimate=pl.CostEstimate(
            flops=4 * n * rows * depth * cols,
            bytes_accessed=2 * n * depth * (rows + 2 * cols),
            transcendentals=rows * cols,
        ),
        name="hidden",
    )(order, *blocks, gate_proj, up_proj)


def down_kernel(pairs, *refs):
    outs = refs[2 * pairs :]
    n, width = outs[0].shape

    @pl.loop(0, width // TILE)
    def _(k):
        at = pl.ds(pl.multiple_of(k * TILE, TILE), TILE)
        total = jnp.dot(refs[0][...], refs[pairs][:, at], preferred_element_type=F32)
        for i in range(1, pairs):
            total += jnp.dot(refs[i][...], refs[pairs + i][:, at], preferred_element_type=F32)
        for i, out in enumerate(outs):
            out[:, at] = total[i * n : (i + 1) * n].astype(BF16)


def down_of(hiddens, downs):
    rows, inner = hiddens[0].shape
    width = downs[0].shape[1]
    n = len(hiddens)
    size = NZ * SLOTS
    outs = rows // size
    return pl.pallas_call(
        functools.partial(down_kernel, n),
        in_specs=[vmem()] * (2 * n),
        out_specs=[vmem()] * outs,
        out_shape=[jax.ShapeDtypeStruct((size, width), BF16)] * outs,
        cost_estimate=pl.CostEstimate(
            flops=2 * n * rows * inner * width,
            bytes_accessed=2 * n * inner * (rows + width) + 2 * rows * width,
            transcendentals=0,
        ),
        name="down",
    )(*hiddens, *downs)


def combine_kernel(high_ref, low_ref, *refs):
    rows, outs = refs[:NEAR], refs[NEAR:]
    n, width = outs[0].shape

    @pl.loop(0, width // TILE)
    def _(i):
        at = pl.ds(pl.multiple_of(i * TILE, TILE), TILE)
        block = jnp.concatenate([r[:, at] for r in rows])
        total = jnp.dot(high_ref[...], block, preferred_element_type=F32)
        total += jnp.dot(low_ref[...], block, preferred_element_type=F32)
        for k in range(NZ):
            outs[k][:, at] = total[k * n : (k + 1) * n].astype(BF16)


def combine_of(high, low, rows):
    width = rows[0].shape[1]
    count = high.shape[0] // NZ
    return pl.pallas_call(
        combine_kernel,
        in_specs=[vmem()] * (2 + NEAR),
        out_specs=[vmem()] * NZ,
        out_shape=[jax.ShapeDtypeStruct((count, width), BF16)] * NZ,
        cost_estimate=pl.CostEstimate(
            flops=10**9, bytes_accessed=4 * 10**6, transcendentals=0
        ),
        name="combine",
    )(high, low, *rows)


def ep_of(x, z, c):
    return (x % NX * NZ + z % NZ) * NC + c % NC


PLACES = [(x, z, c) for x in range(NX) for z in range(NZ) for c in range(NC)]


def over_z(value, by):
    return lax.ppermute(value, "ep", [(ep_of(x, z, c), ep_of(x, z + by, c)) for x, z, c in PLACES])


def over_xc(value, dx, dc):
    return lax.ppermute(value, "ep", [(ep_of(x, z, c), ep_of(x + dx, z, c + dc)) for x, z, c in PLACES])


def layer(tokens, routes, route_weights, gate_proj, up_proj, down_proj):
    w_down = down_proj[0]
    width = tokens.shape[1]
    parts = lax.axis_size("tp")
    tp = lax.axis_index("tp")
    ep = lax.axis_index("ep")
    x, z, c = ep // (NZ * NC), ep // NC % NZ, ep % NC
    near_steps = [(dx, dc) for dc in range(NC) for dx in range(NX)]
    near = jnp.stack([ep_of(x + dx, z, c + dc) for dx, dc in near_steps]).astype(jnp.int32)
    order = jnp.stack([(tp + by) % parts for by in (0, parts - 1, 1, 2)]).astype(jnp.int32)

    def over_y(value, by):
        return lax.ppermute(value, "tp", [(i, (i + by) % parts) for i in range(parts)])

    high = lax.reduce_precision(route_weights, 8, 7)
    meta = jnp.concatenate([routes.astype(F32), high, route_weights - high], axis=1)
    meta = jnp.pad(meta, ((0, 0), (0, META - meta.shape[1]))).astype(BF16)
    tagged = jnp.concatenate([tokens, meta], axis=1)
    pieces = [tagged] + [over_z(tagged, by) for by in range(1, NZ)]

    downs = []
    for by in range(parts):
        start = (tp + by) % parts * width
        piece = lax.dynamic_slice_in_dim(w_down, start, width, axis=1)
        downs.append(piece if by == 0 else over_y(piece, by))

    sent = select_of(near, pieces, width)
    arrived = [v if (dx, dc) == (0, 0) else over_xc(v, dx, dc) for v, (dx, dc) in zip(sent, near_steps)]
    weights_high, weights_low = weigh_of(near, pieces)

    half = NEAR // 2
    returned = []
    for side in range(2):
        mine = jnp.concatenate(arrived[side * half : (side + 1) * half])
        left = over_y(mine, 1)
        right = over_y(mine, -1)
        across = over_y(left, 1) if side == 0 else over_y(right, -1)
        hidden = hidden_of(order, [mine, left, right, across], gate_proj, up_proj)
        hiddens = [hidden] + [over_y(hidden, by) for by in range(1, parts)]
        out = down_of(hiddens, downs)
        for v, (dx, dc) in zip(out, near_steps[side * half : (side + 1) * half]):
            returned.append(v if (dx, dc) == (0, 0) else over_xc(v, -dx, -dc))

    mixed = combine_of(weights_high, weights_low, returned)
    shares = [mixed[0]] + [over_z(mixed[by], -by) for by in range(1, NZ)]
    total = shares[0].astype(F32)
    for share in shares[1:]:
        total = total + share.astype(F32)
    return total.astype(BF16)


def solution(mesh):
    in_specs = (
        P("ep", "tp"),
        P("ep", None),
        P("ep", None),
        P("ep", None, "tp"),
        P("ep", None, "tp"),
        P("ep", "tp", None),
    )
    out_specs = P("ep", "tp")
    return jax.shard_map(layer, mesh=mesh, in_specs=in_specs, out_specs=out_specs, check_vma=False)
```

```python
import functools

import jax
import jax.numpy as jnp
from jax import lax
from jax.experimental import pallas as pl
from jax.experimental.pallas import tpu as pltpu
from jax.sharding import Mesh
from jax.sharding import PartitionSpec as P


NX, NZ, NC = 4, 8, 2
NEAR = NX * NC
SLOTS = 8
HALF = NZ // 2
META = 128
TILE = 256
F32 = jnp.float32
BF16 = jnp.bfloat16


def smem():
    return pl.BlockSpec(memory_space=pltpu.SMEM)


def vmem():
    return pl.BlockSpec(memory_space=pltpu.VMEM)


def tag_kernel(tokens_ref, routes_ref, weights_ref, out_ref):
    copies, rows, wide = out_ref.shape
    width = tokens_ref.shape[1]
    weights = weights_ref[...]
    high = weights.astype(BF16).astype(F32)
    ids = routes_ref[...].astype(F32)
    rest = jnp.zeros((rows, wide - width - 3 * ids.shape[1]), F32)
    meta = jnp.concatenate([ids, high, weights - high, rest], axis=1).astype(BF16)
    for k in range(copies):
        out_ref[k, :, :width] = tokens_ref[...]
        out_ref[k, :, width:] = meta


def tag_of(tokens, routes, weights):
    rows, width = tokens.shape
    return pl.pallas_call(
        tag_kernel,
        in_specs=[vmem()] * 3,
        out_specs=vmem(),
        out_shape=jax.ShapeDtypeStruct((NZ, rows, width + META), BF16),
        name="tag",
    )(tokens, routes, weights)


def placing(experts_ref, meta):
    count = meta.shape[0]
    lane = lax.broadcasted_iota(jnp.int32, meta.shape, 1)
    hits = jnp.zeros(meta.shape, F32)
    eqs = []
    for q in range(NEAR):
        eq = (meta == experts_ref[q].astype(F32)) & (lane < SLOTS)
        eqs.append(eq)
        hit = jnp.max(jnp.where(eq, 1.0, 0.0), axis=1, keepdims=True)
        hits = jnp.where(lane == q, hit, hits)
    block = count // NZ
    r = lax.broadcasted_iota(jnp.int32, (count, count), 0)
    c = lax.broadcasted_iota(jnp.int32, (count, count), 1)
    earlier = jnp.where((r // block == c // block) & (c < r), 1.0, 0.0).astype(BF16)
    slots = jnp.dot(earlier, hits.astype(BF16), preferred_element_type=F32)
    return eqs, jnp.where(hits > 0.5, slots, -1.0)


def spread(values, slots, half):
    group = HALF * SLOTS
    count = slots.shape[0] // 2
    shape = (count, 4 * group)
    lane = lax.broadcasted_iota(jnp.int32, shape, 1)
    row = lax.broadcasted_iota(jnp.int32, shape, 0)
    same = (lane % group) // SLOTS == row // (count // HALF)
    column = (lane % SLOTS).astype(F32)
    parts = []
    for first in range(0, NEAR, 4):
        slot = value = jnp.zeros(shape, F32)
        for i in range(4):
            q = first + i
            here = lane // group == i
            slot = jnp.where(here, slots[half * count : (half + 1) * count, q : q + 1], slot)
            value = jnp.where(here, values[q][half * count : (half + 1) * count], value)
        parts.append(jnp.where(same & (slot == column), value, 0.0))
    return jnp.concatenate(parts, axis=1)


def select_kernel(experts_ref, tagged_ref, *outs):
    count, wide = tagged_ref.shape
    width = wide - META
    _, slots = placing(experts_ref, tagged_ref[:, width:].astype(F32))
    ones = [jnp.ones((count, 1), F32)] * NEAR
    size = count // 2
    masks = [spread(ones, slots, half).T.astype(BF16) for half in range(2)]

    @pl.loop(0, width // TILE)
    def _(i):
        at = pl.ds(pl.multiple_of(i * TILE, TILE), TILE)
        for half in range(2):
            rows = tagged_ref[half * size : (half + 1) * size, at]
            sent = jnp.dot(masks[half], rows, preferred_element_type=F32)
            outs[half][:, at] = sent.astype(BF16)


def select_of(near, tagged):
    rows = NEAR * HALF * SLOTS
    out = jax.ShapeDtypeStruct((rows, tagged.shape[1] - META), BF16)
    return pl.pallas_call(
        select_kernel,
        in_specs=[smem(), vmem()],
        out_specs=[vmem()] * 2,
        out_shape=[out] * 2,
        cost_estimate=pl.CostEstimate(flops=10**9, bytes_accessed=3 * 10**6, transcendentals=0),
        name="select",
    )(near, tagged)


def weigh_kernel(experts_ref, meta_ref, *outs):
    meta = meta_ref[...].astype(F32)
    eqs, slots = placing(experts_ref, meta)
    for order in range(2):
        moved = pltpu.roll(meta, META - (order + 1) * SLOTS, 1)
        values = [jnp.sum(jnp.where(eq, moved, 0.0), axis=1, keepdims=True) for eq in eqs]
        for half in range(2):
            outs[2 * half + order][...] = spread(values, slots, half).astype(BF16)


def weigh_of(near, tagged):
    count, wide = tagged.shape
    out = jax.ShapeDtypeStruct((count // 2, NEAR * HALF * SLOTS), BF16)
    return pl.pallas_call(
        weigh_kernel,
        grid=(1,),
        in_specs=[smem(), pl.BlockSpec((count, META), lambda i: (0, wide // META - 1))],
        out_specs=[pl.BlockSpec(out.shape, lambda i: (0, 0))] * 4,
        out_shape=[out] * 4,
        cost_estimate=pl.CostEstimate(flops=10**9, bytes_accessed=10**6, transcendentals=0),
        name="weigh",
    )(near, tagged)


def hidden_kernel(order_ref, mine, left, right, front, rear, gate_ref, up_ref, out_ref, gate_acc, up_acc):
    step = pl.program_id(0)

    def add(block, rows):
        gate_acc[rows, :] += jnp.dot(block[...], gate_ref[...], preferred_element_type=F32)
        up_acc[rows, :] += jnp.dot(block[...], up_ref[...], preferred_element_type=F32)

    rows = mine.shape[0] // 2
    lower, upper = pl.ds(0, rows), pl.ds(rows, rows)

    @pl.when(step == 0)
    def _():
        gate_acc[...] = jnp.zeros_like(gate_acc)
        up_acc[...] = jnp.zeros_like(up_acc)

    for i, block in enumerate((mine, left, right)):

        @pl.when(step == i)
        def _(block=block):
            add(block, slice(None))

    @pl.when(step == 3)
    def _():
        add(front, lower)
        add(rear, upper)
        gate = gate_acc[...]
        out_ref[...] = (gate / (1.0 + jnp.exp(-gate)) * up_acc[...]).astype(BF16)


def hidden_of(order, blocks, gate_proj, up_proj):
    rows, depth = blocks[0].shape
    cols = gate_proj.shape[2]
    weight = pl.BlockSpec((None, depth, cols), lambda k, order: (0, order[k], 0))
    return pl.pallas_call(
        hidden_kernel,
        grid_spec=pltpu.PrefetchScalarGridSpec(
            num_scalar_prefetch=1,
            grid=(4,),
            in_specs=[pl.BlockSpec(b.shape, lambda k, order: (0, 0)) for b in blocks] + [weight, weight],
            out_specs=pl.BlockSpec((rows, cols), lambda k, order: (0, 0)),
            scratch_shapes=[pltpu.VMEM((rows, cols), F32)] * 2,
        ),
        out_shape=jax.ShapeDtypeStruct((rows, cols), BF16),
        cost_estimate=pl.CostEstimate(
            flops=16 * rows * depth * cols,
            bytes_accessed=8 * depth * (rows + 2 * cols),
            transcendentals=rows * cols,
        ),
        name="hidden",
    )(order, *blocks, gate_proj, up_proj)


def down_kernel(pairs, *refs):
    out = refs[-1]
    hidden = jnp.concatenate([r[...] for r in refs[:pairs]], axis=1)

    @pl.loop(0, out.shape[1] // TILE)
    def _(k):
        at = pl.ds(pl.multiple_of(k * TILE, TILE), TILE)
        weight = jnp.concatenate([r[:, at] for r in refs[pairs : 2 * pairs]])
        out[:, at] = jnp.dot(hidden, weight, preferred_element_type=F32).astype(BF16)


def down_of(hiddens, downs):
    rows, inner = hiddens[0].shape
    width = downs[0].shape[1]
    n = len(hiddens)
    return pl.pallas_call(
        functools.partial(down_kernel, n),
        in_specs=[vmem()] * (2 * n),
        out_specs=vmem(),
        out_shape=jax.ShapeDtypeStruct((rows, width), BF16),
        cost_estimate=pl.CostEstimate(
            flops=2 * n * rows * inner * width,
            bytes_accessed=2 * n * inner * (rows + width) + 2 * rows * width,
            transcendentals=0,
        ),
        name="down",
    )(*hiddens, *downs)


def combine_kernel(*refs):
    weights, rows, out = refs[:4], refs[4:6], refs[6]
    size = weights[0].shape[0]

    @pl.loop(0, out.shape[1] // TILE)
    def _(i):
        at = pl.ds(pl.multiple_of(i * TILE, TILE), TILE)
        for half in range(2):
            block = rows[half][:, at]
            total = jnp.dot(weights[2 * half][...], block, preferred_element_type=F32)
            total += jnp.dot(weights[2 * half + 1][...], block, preferred_element_type=F32)
            out[half * size : (half + 1) * size, at] = total.astype(BF16)


def combine_of(weights, rows):
    count, width = 2 * weights[0].shape[0], rows[0].shape[1]
    return pl.pallas_call(
        combine_kernel,
        in_specs=[vmem()] * 6,
        out_specs=vmem(),
        out_shape=jax.ShapeDtypeStruct((count, width), BF16),
        cost_estimate=pl.CostEstimate(flops=10**9, bytes_accessed=4 * 10**6, transcendentals=0),
        name="combine",
    )(*weights, *rows)


def exchange(value, axes, peers):
    rows = value.shape[0]
    value = value.reshape(peers, rows // peers, value.shape[1])
    return lax.all_to_all(value, axes, split_axis=0, concat_axis=0, tiled=True).reshape(rows, -1)


def layer(tokens, routes, route_weights, gate_proj, up_proj, down_proj):
    w_down = down_proj[0]
    rows, width = tokens.shape
    parts = lax.axis_size("tp")
    tp = lax.axis_index("tp")
    near = (jnp.arange(NEAR, dtype=jnp.int32) // NC * NZ + lax.axis_index("z")) * NC + jnp.arange(
        NEAR, dtype=jnp.int32
    ) % NC
    order = (tp + jnp.array([0, parts - 1, 1, 2], jnp.int32)) % parts

    def over_y(value, by):
        return lax.ppermute(value, "tp", [(i, (i + by) % parts) for i in range(parts)])

    tagged = tag_of(tokens, routes, route_weights).reshape(NZ * rows, width + META)
    tagged = exchange(tagged, "z", NZ)

    downs = []
    for by in range(parts):
        start = (tp + by) % parts * width
        piece = lax.dynamic_slice_in_dim(w_down, start, width, axis=1)
        downs.append(piece if by == 0 else over_y(piece, by))

    sent = select_of(near, tagged)
    mixing = weigh_of(near, tagged)

    returned = []
    for side in range(2):
        mine = exchange(sent[side], ("x", "c"), NEAR)
        cut = mine.shape[0] // 2
        left = over_y(mine, 1)
        right = over_y(mine, -1)
        front = over_y(left[:cut], 1)
        rear = over_y(right[cut:], -1)
        hidden = hidden_of(order, [mine, left, right, front, rear], gate_proj, up_proj)
        hiddens = [hidden] + [over_y(hidden, by) for by in range(1, parts)]
        out = down_of(hiddens, downs)
        returned.append(exchange(out, ("x", "c"), NEAR))

    mixed = combine_of(mixing, returned)
    shares = exchange(mixed, "z", NZ)
    total = jnp.sum(shares.reshape(NZ, rows, width).astype(F32), axis=0)
    return total.astype(BF16)


def solution(mesh):
    ep = ("x", "z", "c")
    parts = mesh.shape["tp"]
    mesh = Mesh(mesh.devices.reshape(NX, NZ, NC, parts), (*ep, "tp"))
    in_specs = (
        P(ep, "tp"),
        P(ep, None),
        P(ep, None),
        P(ep, None, "tp"),
        P(ep, None, "tp"),
        P(ep, "tp", None),
    )
    out_specs = P(ep, "tp")
    return jax.shard_map(layer, mesh=mesh, in_specs=in_specs, out_specs=out_specs, check_vma=False)
```

```python
import functools

import jax
import jax.numpy as jnp
from jax import lax
from jax.experimental import pallas as pl
from jax.experimental.pallas import tpu as pltpu
from jax.sharding import PartitionSpec as P


SIZES = (4, 4)
TILE = 256
F32 = jnp.float32
BF16 = jnp.bfloat16


def vmem():
    return pl.BlockSpec(memory_space=pltpu.VMEM)


def hidden_kernel(order_ref, mine, left, right, front, rear, gate_ref, up_ref, out_ref, gate_acc, up_acc):
    step = pl.program_id(0)

    def add(block, rows):
        gate_acc[rows, :] += jnp.dot(block[...], gate_ref[...], preferred_element_type=F32)
        up_acc[rows, :] += jnp.dot(block[...], up_ref[...], preferred_element_type=F32)

    rows = mine.shape[0] // 2
    lower, upper = pl.ds(0, rows), pl.ds(rows, rows)

    @pl.when(step == 0)
    def _():
        gate_acc[...] = jnp.zeros_like(gate_acc)
        up_acc[...] = jnp.zeros_like(up_acc)

    for i, block in enumerate((mine, left, right)):

        @pl.when(step == i)
        def _(block=block):
            add(block, slice(None))

    @pl.when(step == 3)
    def _():
        add(front, lower)
        add(rear, upper)
        gate = gate_acc[...]
        out_ref[...] = (gate / (1.0 + jnp.exp(-gate)) * up_acc[...]).astype(BF16)


def hidden_of(order, blocks, gate_proj, up_proj):
    rows, depth = blocks[0].shape
    cols = gate_proj.shape[2]
    weight = pl.BlockSpec((None, depth, cols), lambda k, order: (0, order[k], 0))
    return pl.pallas_call(
        hidden_kernel,
        grid_spec=pltpu.PrefetchScalarGridSpec(
            num_scalar_prefetch=1,
            grid=(4,),
            in_specs=[pl.BlockSpec(b.shape, lambda k, order: (0, 0)) for b in blocks] + [weight, weight],
            out_specs=pl.BlockSpec((rows, cols), lambda k, order: (0, 0)),
            scratch_shapes=[pltpu.VMEM((rows, cols), F32)] * 2,
        ),
        out_shape=jax.ShapeDtypeStruct((rows, cols), BF16),
        cost_estimate=pl.CostEstimate(
            flops=16 * rows * depth * cols,
            bytes_accessed=8 * depth * (rows + 2 * cols),
            transcendentals=rows * cols,
        ),
        name="hidden",
    )(order, *blocks, gate_proj, up_proj)


def down_kernel(pairs, *refs):
    out = refs[-1]
    hidden = jnp.concatenate([r[...] for r in refs[:pairs]], axis=1)

    @pl.loop(0, out.shape[1] // TILE)
    def _(k):
        at = pl.ds(pl.multiple_of(k * TILE, TILE), TILE)
        weight = jnp.concatenate([r[:, at] for r in refs[pairs : 2 * pairs]])
        out[:, at] = jnp.dot(hidden, weight, preferred_element_type=F32).astype(BF16)


def down_of(hiddens, downs):
    rows, inner = hiddens[0].shape
    width = downs[0].shape[1]
    n = len(hiddens)
    return pl.pallas_call(
        functools.partial(down_kernel, n),
        in_specs=[vmem()] * (2 * n),
        out_specs=vmem(),
        out_shape=jax.ShapeDtypeStruct((rows, width), BF16),
        cost_estimate=pl.CostEstimate(
            flops=2 * n * rows * inner * width,
            bytes_accessed=2 * n * inner * (rows + width) + 2 * rows * width,
            transcendentals=0,
        ),
        name="down",
    )(*hiddens, *downs)


def layer(tokens, routes, route_weights, gate_proj, up_proj, down_proj):
    w_down = down_proj[0]
    tok_count, width = tokens.shape
    fanout = routes.shape[1]
    experts = lax.axis_size("ep")
    parts = lax.axis_size("tp")
    tp = lax.axis_index("tp")
    capacity = sum(SIZES)
    order = (tp + jnp.array([0, parts - 1, 1, 2], jnp.int32)) % parts

    def over_y(value, by):
        return lax.ppermute(value, "tp", [(i, (i + by) % parts) for i in range(parts)])

    def exchange(value):
        blocks = value.reshape(experts, value.shape[0] // experts, width)
        blocks = lax.all_to_all(blocks, "ep", split_axis=0, concat_axis=0, tiled=True)
        return blocks.reshape(value.shape)

    downs = []
    for by in range(parts):
        start = (tp + by) % parts * width
        piece = lax.dynamic_slice_in_dim(w_down, start, width, axis=1)
        downs.append(piece if by == 0 else over_y(piece, by))

    flat_ids = routes.reshape(-1)
    onehot = (flat_ids[:, None] == jnp.arange(experts, dtype=jnp.int32)[None, :]).astype(jnp.int32)
    before = jnp.cumsum(onehot, axis=0) - onehot
    position = jnp.sum(before * onehot, axis=1)
    target = (flat_ids * capacity + position).reshape(tok_count, fanout)

    mixed = jnp.zeros((tok_count, width), F32)
    first = 0
    for size in SIZES:
        row = jnp.arange(experts * size, dtype=jnp.int32)
        slot = row // size * capacity + first + row % size
        first += size
        select = jnp.any(target[None, :, :] == slot[:, None, None], axis=2).astype(BF16)
        sending = jnp.dot(select, tokens, preferred_element_type=F32).astype(BF16)
        mine = exchange(sending)
        cut = mine.shape[0] // 2
        left = over_y(mine, 1)
        right = over_y(mine, -1)
        front = over_y(left[:cut], 1)
        rear = over_y(right[cut:], -1)
        hidden = hidden_of(order, [mine, left, right, front, rear], gate_proj, up_proj)
        hiddens = [hidden] + [over_y(hidden, by) for by in range(1, parts)]
        out = down_of(hiddens, downs)
        back = exchange(out)
        weight = jnp.sum(
            jnp.where(target[:, :, None] == slot[None, None, :], route_weights[:, :, None], 0.0), axis=1
        )
        high = lax.reduce_precision(weight, 8, 7)
        both = jnp.concatenate([high, weight - high]).astype(BF16)
        both = jnp.dot(both, back, preferred_element_type=F32)
        mixed = mixed + (both[:tok_count] + both[tok_count:])
    return mixed.astype(BF16)


def solution(mesh):
    in_specs = (
        P("ep", "tp"),
        P("ep", None),
        P("ep", None),
        P("ep", None, "tp"),
        P("ep", None, "tp"),
        P("ep", "tp", None),
    )
    out_specs = P("ep", "tp")
    return jax.shard_map(layer, mesh=mesh, in_specs=in_specs, out_specs=out_specs, check_vma=False)
```

```python
import functools

import jax
import jax.numpy as jnp
from jax import lax
from jax.experimental import pallas as pl
from jax.experimental.pallas import tpu as pltpu
from jax.sharding import PartitionSpec as P


SIZES = (4, 4)
F32 = jnp.float32
BF16 = jnp.bfloat16


def vmem():
    return pl.BlockSpec(memory_space=pltpu.VMEM)


def begin_kernel(order_ref, *refs):
    blocks, (gate_ref, up_ref, gate_acc, up_acc) = refs[:3], refs[3:]
    step = pl.program_id(0)

    @pl.when(step == 0)
    def _():
        gate_acc[...] = jnp.zeros_like(gate_acc)
        up_acc[...] = jnp.zeros_like(up_acc)

    for i, block in enumerate(blocks):

        @pl.when(step == i)
        def _(block=block):
            gate_acc[...] += jnp.dot(block[...], gate_ref[...], preferred_element_type=F32)
            up_acc[...] += jnp.dot(block[...], up_ref[...], preferred_element_type=F32)


def finish_kernel(order_ref, front, rear, gate_ref, up_ref, gate_acc, up_acc, out_ref):
    rows = front.shape[0]
    for i, block in enumerate((front, rear)):
        at = pl.ds(i * rows, rows)
        gate = gate_acc[at, :] + jnp.dot(block[...], gate_ref[...], preferred_element_type=F32)
        up = up_acc[at, :] + jnp.dot(block[...], up_ref[...], preferred_element_type=F32)
        out_ref[at, :] = (gate / (1.0 + jnp.exp(-gate)) * up).astype(BF16)


def hidden_of(order, blocks, gate_proj, up_proj):
    rows, depth = blocks[0].shape
    cols = gate_proj.shape[2]
    acc = pl.BlockSpec((rows, cols), lambda k, order: (0, 0))

    def call(kernel, first, count, given, more, outs):
        weight = pl.BlockSpec((None, depth, cols), lambda k, order: (0, order[first + k], 0))
        return pl.pallas_call(
            kernel,
            grid_spec=pltpu.PrefetchScalarGridSpec(
                num_scalar_prefetch=1,
                grid=(count,),
                in_specs=[pl.BlockSpec(b.shape, lambda k, order: (0, 0)) for b in given]
                + [weight, weight]
                + [acc] * len(more),
                out_specs=[acc] * len(outs),
            ),
            out_shape=[jax.ShapeDtypeStruct((rows, cols), t) for t in outs],
            cost_estimate=pl.CostEstimate(
                flops=4 * count * rows * depth * cols,
                bytes_accessed=2 * count * depth * (rows + 2 * cols),
                transcendentals=rows * cols,
            ),
        )(order, *given, gate_proj, up_proj, *more)

    partial = call(begin_kernel, 0, 3, blocks[:3], [], [F32, F32])
    return call(finish_kernel, 3, 1, blocks[3:], partial, [BF16])[0]


def down_kernel(pairs, *refs):
    out = refs[-1]
    experts, share, width = out.shape
    tile = width // 2

    @pl.loop(0, 2)
    def _(k):
        at = pl.ds(pl.multiple_of(k * tile, tile), tile)
        total = jnp.dot(refs[0][...], refs[pairs][:, at], preferred_element_type=F32)
        for i in range(1, pairs):
            total += jnp.dot(refs[i][...], refs[pairs + i][:, at], preferred_element_type=F32)
        out[:, :, at] = total.reshape(experts, share, tile).astype(BF16)


def down_of(hiddens, downs, experts):
    rows, inner = hiddens[0].shape
    width = downs[0].shape[1]
    n = len(hiddens)
    return pl.pallas_call(
        functools.partial(down_kernel, n),
        in_specs=[vmem()] * (2 * n),
        out_specs=vmem(),
        out_shape=jax.ShapeDtypeStruct((experts, rows // experts, width), BF16),
        cost_estimate=pl.CostEstimate(
            flops=2 * n * rows * inner * width,
            bytes_accessed=2 * n * inner * (rows + width) + 2 * rows * width,
            transcendentals=0,
        ),
        name="down",
    )(*hiddens, *downs)


def layer(tokens, routes, route_weights, gate_proj, up_proj, down_proj):
    w_down = down_proj[0]
    tok_count, width = tokens.shape
    fanout = routes.shape[1]
    experts = lax.axis_size("ep")
    parts = lax.axis_size("tp")
    tp = lax.axis_index("tp")
    capacity = sum(SIZES)
    order = (tp + jnp.array([0, parts - 1, 1, 2], jnp.int32)) % parts

    def over_y(value, by):
        return lax.ppermute(value, "tp", [(i, (i + by) % parts) for i in range(parts)])

    def exchange(blocks):
        return lax.all_to_all(blocks, "ep", split_axis=0, concat_axis=0, tiled=True)

    downs = []
    for by in range(parts):
        start = (tp + by) % parts * width
        piece = lax.dynamic_slice_in_dim(w_down, start, width, axis=1)
        downs.append(piece if by == 0 else over_y(piece, by))

    flat_ids = routes.reshape(-1)
    onehot = (flat_ids[:, None] == jnp.arange(experts, dtype=jnp.int32)[None, :]).astype(jnp.int32)
    before = jnp.cumsum(onehot, axis=0) - onehot
    position = jnp.sum(before * onehot, axis=1)
    target = (flat_ids * capacity + position).reshape(tok_count, fanout)

    mixed = jnp.zeros((tok_count, width), F32)
    first = 0
    for size in SIZES:
        row = jnp.arange(experts * size, dtype=jnp.int32)
        slot = row // size * capacity + first + row % size
        first += size
        select = jnp.any(target[None, :, :] == slot[:, None, None], axis=2).astype(BF16)
        sending = jnp.dot(select, tokens, preferred_element_type=F32).astype(BF16)
        landed = exchange(sending.reshape(experts, size, width))
        mine = landed.reshape(-1, width)
        cut = mine.shape[0] // 2
        left = over_y(mine, 1)
        right = over_y(mine, -1)
        left_cut, right_cut = left[:cut], right[cut:]
        front = over_y(left_cut, 1)
        rear = over_y(right_cut, -1)
        hidden = hidden_of(order, [mine, left, right, front, rear], gate_proj, up_proj)
        hiddens = [hidden] + [over_y(hidden, by) for by in range(1, parts)]
        out = down_of(hiddens, downs, experts)
        back = exchange(out).reshape(-1, width)
        weight = jnp.sum(
            jnp.where(target[:, :, None] == slot[None, None, :], route_weights[:, :, None], 0.0), axis=1
        )
        high = lax.reduce_precision(weight, 8, 7)
        both = jnp.concatenate([high, weight - high]).astype(BF16)
        both = jnp.dot(both, back, preferred_element_type=F32)
        mixed = mixed + (both[:tok_count] + both[tok_count:])
    return mixed.astype(BF16)


def solution(mesh):
    in_specs = (
        P("ep", "tp"),
        P("ep", None),
        P("ep", None),
        P("ep", None, "tp"),
        P("ep", None, "tp"),
        P("ep", "tp", None),
    )
    out_specs = P("ep", "tp")
    return jax.shard_map(layer, mesh=mesh, in_specs=in_specs, out_specs=out_specs, check_vma=False)
```

```python
import functools

import jax
import jax.numpy as jnp
from jax import lax
from jax.experimental import pallas as pl
from jax.experimental.pallas import tpu as pltpu
from jax.sharding import PartitionSpec as P


SIZES = (4, 4)
F32 = jnp.float32
BF16 = jnp.bfloat16


def vmem():
    return pl.BlockSpec(memory_space=pltpu.VMEM)


def land_kernel(blocks, *outs):
    experts, share, width = blocks.shape
    half = experts // 2
    for i, out in enumerate(outs):
        part = blocks[i * half : (i + 1) * half].astype(F32)
        out[...] = part.reshape(half * share, width).astype(BF16)


def land_of(blocks):
    experts, share, width = blocks.shape
    rows, cols = experts * share // 2, width // 2
    return pl.pallas_call(
        land_kernel,
        grid=(2,),
        in_specs=[pl.BlockSpec((experts, share, cols), lambda k: (0, 0, k))],
        out_specs=[pl.BlockSpec((rows, cols), lambda k: (0, k))] * 2,
        out_shape=[jax.ShapeDtypeStruct((rows, width), BF16)] * 2,
        cost_estimate=pl.CostEstimate(flops=10**7, bytes_accessed=8 * rows * width, transcendentals=0),
        name="land",
    )(blocks)


def begin_kernel(order_ref, *refs):
    blocks, (gate_ref, up_ref, gate_acc, up_acc) = refs[:6], refs[6:]
    step = pl.program_id(0)

    @pl.when(step == 0)
    def _():
        gate_acc[...] = jnp.zeros_like(gate_acc)
        up_acc[...] = jnp.zeros_like(up_acc)

    for i in range(3):

        @pl.when(step == i)
        def _(i=i):
            block = jnp.concatenate([blocks[2 * i][...], blocks[2 * i + 1][...]])
            gate_acc[...] += jnp.dot(block, gate_ref[...], preferred_element_type=F32)
            up_acc[...] += jnp.dot(block, up_ref[...], preferred_element_type=F32)


def finish_kernel(order_ref, front, rear, gate_ref, up_ref, gate_acc, up_acc, out_ref):
    rows = front.shape[0]
    for i, block in enumerate((front, rear)):
        at = pl.ds(i * rows, rows)
        gate = gate_acc[at, :] + jnp.dot(block[...], gate_ref[...], preferred_element_type=F32)
        up = up_acc[at, :] + jnp.dot(block[...], up_ref[...], preferred_element_type=F32)
        out_ref[at, :] = (gate / (1.0 + jnp.exp(-gate)) * up).astype(BF16)


def hidden_of(order, blocks, gate_proj, up_proj):
    rows, depth = 2 * blocks[0].shape[0], blocks[0].shape[1]
    cols = gate_proj.shape[2]
    acc = pl.BlockSpec((rows, cols), lambda k, order: (0, 0))

    def call(kernel, first, count, given, more, outs):
        weight = pl.BlockSpec((None, depth, cols), lambda k, order: (0, order[first + k], 0))
        return pl.pallas_call(
            kernel,
            grid_spec=pltpu.PrefetchScalarGridSpec(
                num_scalar_prefetch=1,
                grid=(count,),
                in_specs=[pl.BlockSpec(b.shape, lambda k, order: (0, 0)) for b in given]
                + [weight, weight]
                + [acc] * len(more),
                out_specs=[acc] * len(outs),
            ),
            out_shape=[jax.ShapeDtypeStruct((rows, cols), t) for t in outs],
            cost_estimate=pl.CostEstimate(
                flops=4 * count * rows * depth * cols,
                bytes_accessed=2 * count * depth * (rows + 2 * cols),
                transcendentals=rows * cols,
            ),
        )(order, *given, gate_proj, up_proj, *more)

    partial = call(begin_kernel, 0, 3, blocks[:6], [], [F32, F32])
    return call(finish_kernel, 3, 1, blocks[6:], partial, [BF16])[0]


def down_kernel(pairs, *refs):
    out = refs[-1]
    experts, share, width = out.shape
    tile = width // 2

    @pl.loop(0, 2)
    def _(k):
        at = pl.ds(pl.multiple_of(k * tile, tile), tile)
        total = jnp.dot(refs[0][...], refs[pairs][:, at], preferred_element_type=F32)
        for i in range(1, pairs):
            total += jnp.dot(refs[i][...], refs[pairs + i][:, at], preferred_element_type=F32)
        out[:, :, at] = total.reshape(experts, share, tile).astype(BF16)


def down_of(hiddens, downs, experts):
    rows, inner = hiddens[0].shape
    width = downs[0].shape[1]
    n = len(hiddens)
    return pl.pallas_call(
        functools.partial(down_kernel, n),
        in_specs=[vmem()] * (2 * n),
        out_specs=vmem(),
        out_shape=jax.ShapeDtypeStruct((experts, rows // experts, width), BF16),
        cost_estimate=pl.CostEstimate(
            flops=2 * n * rows * inner * width,
            bytes_accessed=2 * n * inner * (rows + width) + 2 * rows * width,
            transcendentals=0,
        ),
        name="down",
    )(*hiddens, *downs)


def layer(tokens, routes, route_weights, gate_proj, up_proj, down_proj):
    w_down = down_proj[0]
    tok_count, width = tokens.shape
    fanout = routes.shape[1]
    experts = lax.axis_size("ep")
    parts = lax.axis_size("tp")
    tp = lax.axis_index("tp")
    capacity = sum(SIZES)
    order = (tp + jnp.array([0, parts - 1, 1, 2], jnp.int32)) % parts

    def over_y(value, by):
        return lax.ppermute(value, "tp", [(i, (i + by) % parts) for i in range(parts)])

    def exchange(blocks):
        return lax.all_to_all(blocks, "ep", split_axis=0, concat_axis=0, tiled=True)

    def piece(source, by):
        return lax.dynamic_slice_in_dim(source, (tp + by) % parts * width, width, axis=1)

    after, before_it = over_y(piece(w_down, 1), 1), over_y(piece(w_down, -1), -1)

    flat_ids = routes.reshape(-1)
    onehot = (flat_ids[:, None] == jnp.arange(experts, dtype=jnp.int32)[None, :]).astype(jnp.int32)
    before = jnp.cumsum(onehot, axis=0) - onehot
    position = jnp.sum(before * onehot, axis=1)
    target = (flat_ids * capacity + position).reshape(tok_count, fanout)

    selections = []
    first = 0
    for size in SIZES:
        row = jnp.arange(experts * size, dtype=jnp.int32)
        slot = row // size * capacity + first + row % size
        first += size
        select = jnp.any(target[None, :, :] == slot[:, None, None], axis=2).astype(BF16)
        sending = jnp.dot(select, tokens, preferred_element_type=F32).astype(BF16)
        selections.append((slot, sending.reshape(experts, size, width)))

    w_late, last_sending = lax.optimization_barrier((w_down, selections[-1][1]))
    selections[-1] = (selections[-1][0], last_sending)
    opposite = over_y(piece(w_late, 2), 2)
    downs = [piece(w_late, 0), after, opposite, before_it]

    mixed = jnp.zeros((tok_count, width), F32)
    for slot, sending in selections:
        landed = exchange(sending)
        mine = land_of(landed)
        left = [over_y(mine[0], 1)]
        right = [over_y(mine[1], -1)]
        left.append(over_y(mine[1], 1))
        right.insert(0, over_y(mine[0], -1))
        front = over_y(left[0], 1)
        rear = over_y(right[1], -1)
        hidden = hidden_of(order, [*mine, *left, *right, front, rear], gate_proj, up_proj)
        hiddens = [hidden] + [over_y(hidden, by) for by in range(1, parts)]
        out = down_of(hiddens, downs, experts)
        back = exchange(out).reshape(-1, width)
        weight = jnp.sum(
            jnp.where(target[:, :, None] == slot[None, None, :], route_weights[:, :, None], 0.0), axis=1
        )
        high = lax.reduce_precision(weight, 8, 7)
        both = jnp.concatenate([high, weight - high]).astype(BF16)
        both = jnp.dot(both, back, preferred_element_type=F32)
        mixed = mixed + (both[:tok_count] + both[tok_count:])
    return mixed.astype(BF16)


def solution(mesh):
    in_specs = (
        P("ep", "tp"),
        P("ep", None),
        P("ep", None),
        P("ep", None, "tp"),
        P("ep", None, "tp"),
        P("ep", "tp", None),
    )
    out_specs = P("ep", "tp")
    return jax.shard_map(layer, mesh=mesh, in_specs=in_specs, out_specs=out_specs, check_vma=False)
```
